128 devices in a mesh: dp: 1, ep: 128 (over z, y, x, core).
Axes of the slice: x: 4, y: 4, z: 4, core: 2. Of those that a mesh axis runs over, the one named last changes fastest.
Arguments:
- tokens: bfloat16 [65536, 2048], P(('dp', 'ep'))
- choice_idx: int32 [128, 1024], P(('dp', 'ep'))
- gate_weight: float32 [128, 1024], P(('dp', 'ep'))
- w_in: bfloat16 [128, 2048, 768], P('ep')
- w_out: bfloat16 [128, 768, 2048], P('ep')
Outputs:
- output: bfloat16 [65536, 2048], P(('dp', 'ep'))
All inputs are finite; a program needn't handle non-finite values.
Results may differ from the reference program's by a relative error of at most 0.00638937.
Values are sent between devices in bfloat16 or wider.
A program may use at most 1 GiB of HBM per device.

```python
import jax
import jax.numpy as jnp
from jax import lax

D_MODEL = 2048
D_FF = 768
EXPERTS = 128
TOKENS = 65536
CAPACITY = 1024
GROUP_SIZE = 128


def draw_routing(route_key):
    tok_local = TOKENS // GROUP_SIZE
    slots_dev = (EXPERTS // GROUP_SIZE) * CAPACITY
    base_share = slots_dev // GROUP_SIZE
    hot_rows = tok_local // 8
    cold_rows = tok_local - hot_rows
    half_group = GROUP_SIZE // 2
    route_keys = jax.random.split(route_key, 6)
    dev_grid = jnp.tile(jnp.arange(GROUP_SIZE, dtype=jnp.int32)[None, :], (GROUP_SIZE, 1))
    src_perm = jax.random.permutation(route_keys[0], dev_grid, axis=1, independent=True)
    pair_delta = jax.random.randint(route_keys[1], (GROUP_SIZE, half_group), 0, base_share + 1)
    pair_delta = pair_delta.at[:, 0].set(base_share)
    perm_counts = jnp.stack([base_share + pair_delta, base_share - pair_delta], axis=2).reshape(GROUP_SIZE, GROUP_SIZE)
    dest_ids = jnp.arange(GROUP_SIZE)[:, None]
    counts = jnp.zeros((GROUP_SIZE, GROUP_SIZE), jnp.int32).at[dest_ids, src_perm].set(perm_counts)
    block_ends = jnp.cumsum(counts, axis=1)
    starts = block_ends - counts
    slot_pos = jnp.arange(slots_dev, dtype=jnp.int32)
    src_of = jax.vmap(lambda end_row: jnp.searchsorted(end_row, slot_pos, side="right"))(block_ends)
    within = slot_pos[None, :] - jnp.take_along_axis(starts, src_of, axis=1)
    block_len = jnp.take_along_axis(counts, src_of, axis=1)
    hot_count = jnp.minimum(block_len // 2, hot_rows)
    hot_off = jax.random.randint(route_keys[2], (GROUP_SIZE, GROUP_SIZE), 0, hot_rows)
    cold_off = jax.random.randint(route_keys[3], (GROUP_SIZE, GROUP_SIZE), 0, cold_rows)
    hot_pick = (jnp.take_along_axis(hot_off, src_of, axis=1) + within) % hot_rows
    cold_pick = hot_rows + (jnp.take_along_axis(cold_off, src_of, axis=1) + within - hot_count) % cold_rows
    local_rank = jnp.where(within < hot_count, hot_pick, cold_pick)
    row_grid = jnp.tile(jnp.arange(tok_local, dtype=jnp.int32)[None, :], (GROUP_SIZE, 1))
    row_order = jax.random.permutation(route_keys[4], row_grid, axis=1, independent=True).reshape(-1)
    chosen = src_of * tok_local + row_order[src_of * tok_local + local_rank]
    chosen = chosen.reshape(EXPERTS, CAPACITY)
    return jax.random.permutation(route_keys[5], chosen, axis=1, independent=True)


def setup_inputs(seed: int = 0, part: int = 0) -> dict:
    base_key = jax.random.key(seed)
    shared_keys = jax.random.split(base_key, 2)
    part_keys = jax.random.split(jax.random.fold_in(base_key, part), 3)
    tokens = jax.random.normal(part_keys[0], (TOKENS, D_MODEL), jnp.float32).astype(jnp.bfloat16)
    choice_idx = draw_routing(part_keys[1])
    gate_weight = jax.random.uniform(part_keys[2], (EXPERTS, CAPACITY), jnp.float32, 0.5, 1.5)
    w_in = (jax.random.normal(shared_keys[0], (EXPERTS, D_MODEL, D_FF), jnp.float32) * D_MODEL ** -0.5).astype(jnp.bfloat16)
    w_out = (jax.random.normal(shared_keys[1], (EXPERTS, D_FF, D_MODEL), jnp.float32) * D_FF ** -0.5).astype(jnp.bfloat16)
    return {"tokens": tokens, "choice_idx": choice_idx, "gate_weight": gate_weight, "w_in": w_in, "w_out": w_out}


def reference(tokens, choice_idx, gate_weight, w_in, w_out):
    def expert_step(acc_sum, per_expert):
        idx_row, gate_row, w_first, w_second = per_expert
        tok_rows = tokens[idx_row]
        pre_act = jnp.dot(tok_rows, w_first, preferred_element_type=jnp.float32)
        hidden = jax.nn.gelu(pre_act, approximate=True).astype(jnp.bfloat16)
        expert_out = jnp.dot(hidden, w_second, preferred_element_type=jnp.float32)
        weighted = (gate_row[:, None] * expert_out).astype(jnp.bfloat16)
        return acc_sum.at[idx_row].add(weighted.astype(jnp.float32)), None

    zero_acc = jnp.zeros((TOKENS, D_MODEL), jnp.float32)
    acc_sum = lax.scan(expert_step, zero_acc, (choice_idx, gate_weight, w_in, w_out))[0]
    return (tokens.astype(jnp.float32) + acc_sum).astype(jnp.bfloat16)
```

```python
import functools

import jax
import jax.numpy as jnp
from jax import lax
from jax.experimental import pallas as pl
from jax.experimental.pallas import tpu as pltpu
from jax.sharding import PartitionSpec as P

MESH = pl.DeviceIdType.MESH
HIGHEST = lax.Precision.HIGHEST
PEERS = 8
LANES = 128


def _dot(a, b, dims=((1,), (0,)), precision=None):
    return lax.dot_general(a, b, (dims, ((), ())), precision=precision, preferred_element_type=jnp.float32)


def moe_kernel(n, sel_ref, gate_ref, tok_hbm, win_hbm, wout_hbm, out_ref,
               tok, win, wout, ask_out, ask_in, gates, rows_out, rows_in, back_out, back_in, acc,
               load_sem, ask_send, ask_recv, rows_send, rows_recv, back_send, back_recv):
    me = lax.axis_index("ep")
    groups = n // PEERS
    my_group = me // PEERS
    pair_cap = LANES // PEERS
    tok_count, model_dim = tok.shape
    slots = sel_ref.shape[1]

    loads = [
        pltpu.make_async_copy(src, dst, load_sem.at[i])
        for i, (src, dst) in enumerate(((tok_hbm, tok), (win_hbm, win), (wout_hbm, wout)))
    ]
    for load in loads:
        load.start()

    barrier = pltpu.get_barrier_semaphore()

    @pl.loop(1, n)
    def _(k):
        pl.semaphore_signal(barrier, inc=1, device_id={"ep": (me + k) % n}, device_id_type=MESH)

    shift = tok_count.bit_length() - 1
    upper = (lax.broadcasted_iota(jnp.int32, (LANES, LANES), 0)
             < lax.broadcasted_iota(jnp.int32, (LANES, LANES), 1)).astype(jnp.bfloat16)
    lane_of = lax.broadcasted_iota(jnp.int32, (LANES, LANES), 0) % pair_cap
    before = jnp.zeros((n, 1), jnp.float32)
    asks = jnp.zeros((n, LANES), jnp.float32)
    weights = jnp.zeros((n, LANES), jnp.float32)
    for b in range(slots // LANES):
        part = slice(b * LANES, (b + 1) * LANES)
        sel = sel_ref[:, part]
        dev = lax.shift_right_logical(sel, shift)
        row = (sel & (tok_count - 1)).astype(jnp.float32) + 1.0
        hot = lax.broadcasted_iota(jnp.int32, (n, LANES), 0) == dev
        hot_f = hot.astype(jnp.float32)
        count = _dot(hot_f.astype(jnp.bfloat16), upper) + before
        before = before + jnp.sum(hot_f, axis=1, keepdims=True)
        rank = jnp.sum(hot_f * count, axis=0, keepdims=True).astype(jnp.int32)
        mine = lane_of == rank
        asks = asks + _dot(hot_f, jnp.where(mine, row, 0.0), ((1,), (1,)), HIGHEST)
        weights = weights + _dot(hot_f, jnp.where(mine, gate_ref[:, part], 0.0), ((1,), (1,)), HIGHEST)
    gates[...] = weights
    ask_out[...] = asks.reshape(n, 1, LANES)

    pl.semaphore_wait(barrier, n - 1)

    @pl.loop(1, n)
    def _(k):
        peer = (me + k) % n
        pltpu.make_async_remote_copy(
            src_ref=ask_out.at[peer], dst_ref=ask_in.at[me], send_sem=ask_send, recv_sem=ask_recv,
            device_id={"ep": peer}, device_id_type=MESH).start()

    pltpu.make_async_copy(ask_out.at[me], ask_in.at[me], ask_recv).start()

    pltpu.make_async_copy(ask_in, ask_in, ask_recv).wait()
    for load in loads:
        load.wait()

    own_lanes = (lax.broadcasted_iota(jnp.int32, (PEERS, LANES), 1) // pair_cap
                 == lax.broadcasted_iota(jnp.int32, (PEERS, LANES), 0))

    def lane_row(block):
        return jnp.sum(jnp.where(own_lanes, block, 0.0), axis=0, keepdims=True)

    def column(line):
        return jnp.transpose(jnp.broadcast_to(line, (LANES, LANES)))

    def asked(group):
        return lane_row(ask_in[pl.ds(group * PEERS, PEERS)].reshape(PEERS, LANES))

    def push(src, dst, group, send_sem, recv_sem):
        for i in range(PEERS):
            peer = group * PEERS + i

            @pl.when(peer != me)
            def _():
                pltpu.make_async_remote_copy(
                    src_ref=src.at[peer], dst_ref=dst.at[me], send_sem=send_sem, recv_sem=recv_sem.at[my_group],
                    device_id={"ep": peer}, device_id_type=MESH).start()

            @pl.when(peer == me)
            def _():
                pltpu.make_async_copy(src.at[me], dst.at[me], recv_sem.at[my_group]).start()

    def arrived(dst, group, recv_sem):
        blocks = dst.at[pl.ds(group * PEERS, PEERS)]
        pltpu.make_async_copy(blocks, blocks, recv_sem.at[group]).wait()

    def later(j):
        return (my_group + j) % groups

    def earlier(j):
        return (my_group + groups - j) % groups

    row_ids = lax.broadcasted_iota(jnp.int32, (LANES, tok_count), 1).astype(jnp.float32) + 1.0

    @pl.loop(0, groups)
    def _(j):
        group = later(j)
        want = column(asked(group))
        pick = (jnp.concatenate([want] * (tok_count // LANES), axis=1) == row_ids).astype(jnp.bfloat16)
        for c in range(0, model_dim, 512):
            got = _dot(pick, tok[:, c:c + 512]).astype(jnp.bfloat16)
            rows_out[pl.ds(group * PEERS, PEERS), :, c:c + 512] = got.reshape(PEERS, pair_cap, 512)
        push(rows_out, rows_in, group, rows_send, rows_recv)

    @pl.loop(0, groups)
    def _(j):
        group = earlier(j)
        arrived(rows_in, group, rows_recv)
        first = pl.ds(group * PEERS, PEERS)
        x = rows_in[first].reshape(LANES, model_dim)
        hidden = jax.nn.gelu(_dot(x, win[...]), approximate=True).astype(jnp.bfloat16)
        scale = column(lane_row(gates[pl.ds(pl.multiple_of(group * PEERS, PEERS), PEERS), :]))
        scale = jnp.concatenate([scale] * (512 // LANES), axis=1)
        for c in range(0, model_dim, 512):
            o = _dot(hidden, wout[:, c:c + 512])
            p = jnp.where(scale > 0.0, scale * o, 0.0).astype(jnp.bfloat16)
            back_out[first, :, c:c + 512] = p.reshape(PEERS, pair_cap, 512)
        push(back_out, back_in, group, back_send, back_recv)

    token_ids = lax.broadcasted_iota(jnp.int32, (tok_count, LANES), 0).astype(jnp.float32) + 1.0

    for c in range(0, model_dim, 512):
        acc[:, c:c + 512] = tok[:, c:c + 512].astype(jnp.float32)

    @pl.loop(0, groups)
    def _(j):
        group = later(j)
        put = (token_ids == asked(group)).astype(jnp.bfloat16)
        arrived(back_in, group, back_recv)
        for c in range(0, model_dim, 512):
            p = back_in[pl.ds(group * PEERS, PEERS), :, c:c + 512].reshape(LANES, 512)
            acc[:, c:c + 512] += _dot(put, p)

    for c in range(0, model_dim, 512):
        out_ref[:, c:c + 512] = acc[:, c:c + 512].astype(out_ref.dtype)

    for src, send_sem in ((ask_out, ask_send), (rows_out, rows_send), (back_out, back_send)):
        sent = src.at[pl.ds(0, n - 1)]
        pltpu.make_async_copy(sent, sent, send_sem).wait()


def solution(mesh):
    n = mesh.shape["ep"]
    row_spec = P(("dp", "ep"), None)
    expert_spec = P("ep", None, None)

    def local_layer(tok_loc, sel_loc, gate_loc, win_loc, wout_loc):
        tok_count, model_dim = tok_loc.shape
        ff_dim = win_loc.shape[2]
        pair_cap = LANES // PEERS
        blocks = pltpu.VMEM((n, pair_cap, model_dim), jnp.bfloat16)
        vmem = pl.BlockSpec(memory_space=pltpu.VMEM)
        hbm = pl.BlockSpec(memory_space=pl.ANY)
        return pl.pallas_call(
            functools.partial(moe_kernel, n),
            out_shape=jax.ShapeDtypeStruct((tok_count, model_dim), tok_loc.dtype),
            in_specs=[vmem, vmem, hbm, hbm, hbm],
            out_specs=vmem,
            scratch_shapes=[
                pltpu.VMEM((tok_count, model_dim), jnp.bfloat16),
                pltpu.VMEM((model_dim, ff_dim), jnp.bfloat16),
                pltpu.VMEM((ff_dim, model_dim), jnp.bfloat16),
                pltpu.VMEM((n, 1, LANES), jnp.float32),
                pltpu.VMEM((n, 1, LANES), jnp.float32),
                pltpu.VMEM((n, LANES), jnp.float32),
                blocks, blocks, blocks, blocks,
                pltpu.VMEM((tok_count, model_dim), jnp.float32),
                pltpu.SemaphoreType.DMA((3,)),
                pltpu.SemaphoreType.DMA,
                pltpu.SemaphoreType.DMA,
                pltpu.SemaphoreType.DMA,
                pltpu.SemaphoreType.DMA((n // PEERS,)),
                pltpu.SemaphoreType.DMA,
                pltpu.SemaphoreType.DMA((n // PEERS,)),
            ],
            compiler_params=pltpu.CompilerParams(
                collective_id=0, has_side_effects=True, vmem_limit_bytes=63 * 1024 * 1024),
        )(sel_loc, gate_loc, tok_loc, win_loc[0], wout_loc[0])

    return jax.shard_map(local_layer, mesh=mesh, in_specs=(row_spec, row_spec, row_spec, expert_spec, expert_spec), out_specs=row_spec, check_vma=False)
```

```python
import functools

import jax
import jax.numpy as jnp
from jax import lax
from jax.experimental import pallas as pl
from jax.experimental.pallas import tpu as pltpu
from jax.sharding import PartitionSpec as P

MESH = pl.DeviceIdType.MESH
HIGHEST = lax.Precision.HIGHEST
PEERS = 8
LANES = 128


def _dot(a, b, dims=((1,), (0,)), precision=None):
    return lax.dot_general(a, b, (dims, ((), ())), precision=precision, preferred_element_type=jnp.float32)


def moe_kernel(n, sel_ref, gate_ref, tok_hbm, win_hbm, wout_hbm, out_ref,
               tok, win, wout, ask_out, ask_in, gates, rows_out, rows_in, back_out, back_in, acc,
               load_sem, ask_send, ask_recv, rows_send, rows_recv, back_send, back_recv):
    me = lax.axis_index("ep")
    groups = n // PEERS
    pair_cap = LANES // PEERS
    tok_count, model_dim = tok.shape
    slots = sel_ref.shape[1]

    loads = [
        pltpu.make_async_copy(src, dst, load_sem.at[i])
        for i, (src, dst) in enumerate(((tok_hbm, tok), (win_hbm, win), (wout_hbm, wout)))
    ]
    for load in loads:
        load.start()

    ys = min(4, n // 8)
    zs = n // (8 * ys)

    def partner(j, i, sign):
        t, core = i // 2, i % 2
        y_shift, z_shift = j % ys + t, j // ys + 4 - t
        x = (me // 2 + 4 + sign * t) % 4
        y = (me // 8 + 8 + sign * y_shift) % ys
        z = (me // (8 * ys) + 8 + sign * z_shift) % zs
        return ((z * ys + y) * 4 + x) * 2 + (me + core) % 2

    def push(src, dst, j, i, peer, index, send_sem, recv_sem):
        def remote():
            pltpu.make_async_remote_copy(
                src_ref=src.at[index], dst_ref=dst.at[j * PEERS + i], send_sem=send_sem, recv_sem=recv_sem,
                device_id={"ep": peer}, device_id_type=MESH).start()

        def local():
            pltpu.make_async_copy(src.at[index], dst.at[j * PEERS + i], recv_sem).start()

        if i > 0:
            remote()
        else:
            pl.when(j > 0)(remote)
            pl.when(j == 0)(local)

    barrier = pltpu.get_barrier_semaphore()

    @pl.loop(1, n)
    def _(k):
        pl.semaphore_signal(barrier, inc=1, device_id={"ep": (me + k) % n}, device_id_type=MESH)

    shift = tok_count.bit_length() - 1
    upper = (lax.broadcasted_iota(jnp.int32, (LANES, LANES), 0)
             < lax.broadcasted_iota(jnp.int32, (LANES, LANES), 1)).astype(jnp.bfloat16)
    lane_of = lax.broadcasted_iota(jnp.int32, (LANES, LANES), 0) % pair_cap
    before = jnp.zeros((n, 1), jnp.float32)
    asks = jnp.zeros((n, LANES), jnp.float32)
    weights = jnp.zeros((n, LANES), jnp.float32)
    for b in range(slots // LANES):
        part = slice(b * LANES, (b + 1) * LANES)
        sel = sel_ref[:, part]
        dev = lax.shift_right_logical(sel, shift)
        row = (sel & (tok_count - 1)).astype(jnp.float32) + 1.0
        hot = lax.broadcasted_iota(jnp.int32, (n, LANES), 0) == dev
        hot_f = hot.astype(jnp.float32)
        count = _dot(hot_f.astype(jnp.bfloat16), upper) + before
        before = before + jnp.sum(hot_f, axis=1, keepdims=True)
        rank = jnp.sum(hot_f * count, axis=0, keepdims=True).astype(jnp.int32)
        mine = lane_of == rank
        asks = asks + _dot(hot_f, jnp.where(mine, row, 0.0), ((1,), (1,)), HIGHEST)
        weights = weights + _dot(hot_f, jnp.where(mine, gate_ref[:, part], 0.0), ((1,), (1,)), HIGHEST)
    gates[...] = weights.reshape(n, 1, LANES)
    ask_out[...] = asks.reshape(n, 1, LANES)

    pl.semaphore_wait(barrier, n - 1)

    @pl.loop(0, groups)
    def _(j):
        for i in range(PEERS):
            push(ask_out, ask_in, j, i, partner(j, i, -1), partner(j, i, -1), ask_send, ask_recv)

    pltpu.make_async_copy(ask_in, ask_in, ask_recv).wait()
    for load in loads:
        load.wait()

    own_lanes = (lax.broadcasted_iota(jnp.int32, (PEERS, LANES), 1) // pair_cap
                 == lax.broadcasted_iota(jnp.int32, (PEERS, LANES), 0))

    def lane_row(block):
        return jnp.sum(jnp.where(own_lanes, block, 0.0), axis=0, keepdims=True)

    def column(line):
        return jnp.transpose(jnp.broadcast_to(line, (LANES, LANES)))

    def asked(j):
        return lane_row(ask_in[pl.ds(j * PEERS, PEERS)].reshape(PEERS, LANES))

    def arrived(dst, group, recv_sem):
        blocks = dst.at[pl.ds(group * PEERS, PEERS)]
        pltpu.make_async_copy(blocks, blocks, recv_sem.at[group]).wait()

    row_ids = lax.broadcasted_iota(jnp.int32, (LANES, tok_count), 1).astype(jnp.float32) + 1.0

    @pl.loop(0, groups)
    def _(j):
        want = column(asked(j))
        pick = (jnp.concatenate([want] * (tok_count // LANES), axis=1) == row_ids).astype(jnp.bfloat16)
        for c in range(0, model_dim, 512):
            got = _dot(pick, tok[:, c:c + 512]).astype(jnp.bfloat16)
            rows_out[pl.ds(j * PEERS, PEERS), :, c:c + 512] = got.reshape(PEERS, pair_cap, 512)
        for i in range(PEERS):
            push(rows_out, rows_in, j, i, partner(j, i, 1), j * PEERS + i, rows_send, rows_recv.at[j])

    @pl.loop(0, groups)
    def _(j):
        arrived(rows_in, j, rows_recv)
        first = pl.ds(j * PEERS, PEERS)
        x = rows_in[first].reshape(LANES, model_dim)
        hidden = jax.nn.gelu(_dot(x, win[...]), approximate=True).astype(jnp.bfloat16)
        lines = [gates[partner(j, i, -1)] for i in range(PEERS)]
        scale = column(lane_row(jnp.concatenate(lines, axis=0)))
        scale = jnp.concatenate([scale] * (512 // LANES), axis=1)
        for c in range(0, model_dim, 512):
            o = _dot(hidden, wout[:, c:c + 512])
            p = jnp.where(scale > 0.0, scale * o, 0.0).astype(jnp.bfloat16)
            back_out[first, :, c:c + 512] = p.reshape(PEERS, pair_cap, 512)
        for i in range(PEERS):
            push(back_out, back_in, j, i, partner(j, i, -1), j * PEERS + i, back_send, back_recv.at[j])

    token_ids = lax.broadcasted_iota(jnp.int32, (tok_count, LANES), 0).astype(jnp.float32) + 1.0

    for c in range(0, model_dim, 512):
        acc[:, c:c + 512] = tok[:, c:c + 512].astype(jnp.float32)

    @pl.loop(0, groups)
    def _(j):
        put = (token_ids == asked(j)).astype(jnp.bfloat16)
        arrived(back_in, j, back_recv)
        for c in range(0, model_dim, 512):
            p = back_in[pl.ds(j * PEERS, PEERS), :, c:c + 512].reshape(LANES, 512)
            acc[:, c:c + 512] += _dot(put, p)

    for c in range(0, model_dim, 512):
        out_ref[:, c:c + 512] = acc[:, c:c + 512].astype(out_ref.dtype)

    for src, send_sem in ((ask_out, ask_send), (rows_out, rows_send), (back_out, back_send)):
        sent = src.at[pl.ds(0, n - 1)]
        pltpu.make_async_copy(sent, sent, send_sem).wait()


def solution(mesh):
    n = mesh.shape["ep"]
    row_spec = P(("dp", "ep"), None)
    expert_spec = P("ep", None, None)

    def local_layer(tok_loc, sel_loc, gate_loc, win_loc, wout_loc):
        tok_count, model_dim = tok_loc.shape
        ff_dim = win_loc.shape[2]
        pair_cap = LANES // PEERS
        blocks = pltpu.VMEM((n, pair_cap, model_dim), jnp.bfloat16)
        vmem = pl.BlockSpec(memory_space=pltpu.VMEM)
        hbm = pl.BlockSpec(memory_space=pl.ANY)
        return pl.pallas_call(
            functools.partial(moe_kernel, n),
            out_shape=jax.ShapeDtypeStruct((tok_count, model_dim), tok_loc.dtype),
            in_specs=[vmem, vmem, hbm, hbm, hbm],
            out_specs=vmem,
            scratch_shapes=[
                pltpu.VMEM((tok_count, model_dim), jnp.bfloat16),
                pltpu.VMEM((model_dim, ff_dim), jnp.bfloat16),
                pltpu.VMEM((ff_dim, model_dim), jnp.bfloat16),
                pltpu.VMEM((n, 1, LANES), jnp.float32),
                pltpu.VMEM((n, 1, LANES), jnp.float32),
                pltpu.VMEM((n, 1, LANES), jnp.float32),
                blocks, blocks, blocks, blocks,
                pltpu.VMEM((tok_count, model_dim), jnp.float32),
                pltpu.SemaphoreType.DMA((3,)),
                pltpu.SemaphoreType.DMA,
                pltpu.SemaphoreType.DMA,
                pltpu.SemaphoreType.DMA,
                pltpu.SemaphoreType.DMA((n // PEERS,)),
                pltpu.SemaphoreType.DMA,
                pltpu.SemaphoreType.DMA((n // PEERS,)),
            ],
            compiler_params=pltpu.CompilerParams(
                collective_id=0, has_side_effects=True, vmem_limit_bytes=63 * 1024 * 1024),
        )(sel_loc, gate_loc, tok_loc, win_loc[0], wout_loc[0])

    return jax.shard_map(local_layer, mesh=mesh, in_specs=(row_spec, row_spec, row_spec, expert_spec, expert_spec), out_specs=row_spec, check_vma=False)
```

```python
import functools

import jax
import jax.numpy as jnp
from jax import lax
from jax.experimental import pallas as pl
from jax.experimental.pallas import tpu as pltpu
from jax.sharding import PartitionSpec as P

MESH = pl.DeviceIdType.MESH
HIGHEST = lax.Precision.HIGHEST
PEERS = 8
LANES = 128


def _dot(a, b, dims=((1,), (0,)), precision=None):
    return lax.dot_general(a, b, (dims, ((), ())), precision=precision, preferred_element_type=jnp.float32)


def moe_kernel(n, sel_ref, gate_ref, tok_hbm, win_hbm, wout_hbm, out_ref,
               tok, win, wout, ask_out, ask_in, gates, rows_out, rows_in, back_in, relay_a, relay_b, acc,
               load_sem, ask_send, ask_recv, rows_send, rows_recv, back_send, back_recv,
               relay_a_recv, relay_b_recv, pass_send):
    me = lax.axis_index("ep")
    groups = n // PEERS
    pair_cap = LANES // PEERS
    tok_count, model_dim = tok.shape
    slots = sel_ref.shape[1]

    loads = [
        pltpu.make_async_copy(src, dst, load_sem.at[i])
        for i, (src, dst) in enumerate(((tok_hbm, tok), (win_hbm, win), (wout_hbm, wout)))
    ]
    for load in loads:
        load.start()

    ys = min(4, n // 8)
    zs = n // (8 * ys)

    def device(offset, sign):
        dx, dy, dz, core = offset
        x = (me // 2 + 16 + sign * dx) % 4
        y = (me // 8 + 16 + sign * dy) % ys
        z = (me // (8 * ys) + 16 + sign * dz) % zs
        return ((z * ys + y) * 4 + x) * 2 + (me + core) % 2

    def offset_of(j, i):
        t = i // 2
        return t, (j % ys + t) % ys, (j // ys + 4 - t) % zs, i % 2

    def halfway(d):
        return (d // 2) * (1 - d % 2)

    def legs(offset, half):
        core = offset[3]
        first = [(1 - 2 * half) * halfway(d) + half * (d % 2) * d for d in offset[:3]]
        rest = [d - f for d, f in zip(offset[:3], first)]
        return (*first, half * core), (*rest, (1 - half) * core)

    def relayed(offset):
        return halfway(offset[0]) + halfway(offset[1]) + halfway(offset[2])

    def halves(model_dim):
        return [pl.ds(h * (model_dim // 2), model_dim // 2) for h in range(2)]

    def send(src, dst, relay, j, i, sign, send_sem, recv_sem, relay_recv):
        slot = j * PEERS + i
        offset = offset_of(j, i)

        @pl.when((relayed(offset) == 0) & (slot > 0))
        def _():
            pltpu.make_async_remote_copy(
                src_ref=src.at[slot], dst_ref=dst.at[slot], send_sem=send_sem, recv_sem=recv_sem.at[j],
                device_id={"ep": device(offset, sign)}, device_id_type=MESH).start()

        @pl.when(relayed(offset) > 0)
        def _():
            for half, columns in enumerate(halves(model_dim)):
                pltpu.make_async_remote_copy(
                    src_ref=src.at[slot, :, columns], dst_ref=relay.at[slot, :, columns],
                    send_sem=send_sem, recv_sem=relay_recv.at[slot],
                    device_id={"ep": device(legs(offset, half)[0], sign)}, device_id_type=MESH).start()

        if i == 0:
            @pl.when(slot == 0)
            def _():
                pltpu.make_async_copy(src.at[slot], dst.at[slot], recv_sem.at[j]).start()

    def forward(relay, dst, j, i, sign, pass_send, recv_sem, relay_recv):
        slot = j * PEERS + i
        offset = offset_of(j, i)

        @pl.when(relayed(offset) > 0)
        def _():
            pltpu.make_async_copy(relay.at[slot], relay.at[slot], relay_recv.at[slot]).wait()
            for half, columns in enumerate(halves(model_dim)):
                pltpu.make_async_remote_copy(
                    src_ref=relay.at[slot, :, columns], dst_ref=dst.at[slot, :, columns],
                    send_sem=pass_send, recv_sem=recv_sem.at[j],
                    device_id={"ep": device(legs(offset, half)[1], sign)}, device_id_type=MESH).start()

    barrier = pltpu.get_barrier_semaphore()

    @pl.loop(1, n)
    def _(k):
        pl.semaphore_signal(barrier, inc=1, device_id={"ep": (me + k) % n}, device_id_type=MESH)

    shift = tok_count.bit_length() - 1
    upper = (lax.broadcasted_iota(jnp.int32, (LANES, LANES), 0)
             < lax.broadcasted_iota(jnp.int32, (LANES, LANES), 1)).astype(jnp.bfloat16)
    lane_of = lax.broadcasted_iota(jnp.int32, (LANES, LANES), 0) % pair_cap
    before = jnp.zeros((n, 1), jnp.float32)
    asks = jnp.zeros((n, LANES), jnp.float32)
    weights = jnp.zeros((n, LANES), jnp.float32)
    for b in range(slots // LANES):
        part = slice(b * LANES, (b + 1) * LANES)
        sel = sel_ref[:, part]
        dev = lax.shift_right_logical(sel, shift)
        row = (sel & (tok_count - 1)).astype(jnp.float32) + 1.0
        hot = lax.broadcasted_iota(jnp.int32, (n, LANES), 0) == dev
        hot_f = hot.astype(jnp.float32)
        count = _dot(hot_f.astype(jnp.bfloat16), upper) + before
        before = before + jnp.sum(hot_f, axis=1, keepdims=True)
        rank = jnp.sum(hot_f * count, axis=0, keepdims=True).astype(jnp.int32)
        mine = lane_of == rank
        asks = asks + _dot(hot_f, jnp.where(mine, row, 0.0), ((1,), (1,)), HIGHEST)
        weights = weights + _dot(hot_f, jnp.where(mine, gate_ref[:, part], 0.0), ((1,), (1,)), HIGHEST)
    gates[...] = weights.reshape(n, 1, LANES)
    ask_out[...] = asks.reshape(n, 1, LANES)

    pl.semaphore_wait(barrier, n - 1)

    @pl.loop(0, groups)
    def _(j):
        for i in range(PEERS):
            slot = j * PEERS + i
            peer = device(offset_of(j, i), -1)

            @pl.when(slot > 0)
            def _():
                pltpu.make_async_remote_copy(
                    src_ref=ask_out.at[peer], dst_ref=ask_in.at[slot], send_sem=ask_send, recv_sem=ask_recv,
                    device_id={"ep": peer}, device_id_type=MESH).start()

    pltpu.make_async_copy(ask_out.at[me], ask_in.at[0], ask_recv).start()
    pltpu.make_async_copy(ask_in, ask_in, ask_recv).wait()
    for load in loads:
        load.wait()

    own_lanes = (lax.broadcasted_iota(jnp.int32, (PEERS, LANES), 1) // pair_cap
                 == lax.broadcasted_iota(jnp.int32, (PEERS, LANES), 0))

    def lane_row(block):
        return jnp.sum(jnp.where(own_lanes, block, 0.0), axis=0, keepdims=True)

    def column(line):
        return jnp.transpose(jnp.broadcast_to(line, (LANES, LANES)))

    def asked(j):
        return lane_row(ask_in[pl.ds(j * PEERS, PEERS)].reshape(PEERS, LANES))

    def arrived(dst, group, recv_sem):
        blocks = dst.at[pl.ds(group * PEERS, PEERS)]
        pltpu.make_async_copy(blocks, blocks, recv_sem.at[group]).wait()

    row_ids = lax.broadcasted_iota(jnp.int32, (LANES, tok_count), 1).astype(jnp.float32) + 1.0

    @pl.loop(0, groups)
    def _(j):
        want = column(asked(j))
        pick = (jnp.concatenate([want] * (tok_count // LANES), axis=1) == row_ids).astype(jnp.bfloat16)
        for c in range(0, model_dim, 512):
            got = _dot(pick, tok[:, c:c + 512]).astype(jnp.bfloat16)
            rows_out[pl.ds(j * PEERS, PEERS), :, c:c + 512] = got.reshape(PEERS, pair_cap, 512)
        for i in range(PEERS):
            send(rows_out, rows_in, relay_a, j, i, 1, rows_send, rows_recv, relay_a_recv)

    @pl.loop(0, groups)
    def _(j):
        for i in range(PEERS):
            forward(relay_a, rows_in, j, i, 1, pass_send, rows_recv, relay_a_recv)

    @pl.loop(0, groups)
    def _(j):
        arrived(rows_in, j, rows_recv)
        first = pl.ds(j * PEERS, PEERS)
        x = rows_in[first].reshape(LANES, model_dim)
        hidden = jax.nn.gelu(_dot(x, win[...]), approximate=True).astype(jnp.bfloat16)
        lines = [gates[device(offset_of(j, i), -1)] for i in range(PEERS)]
        scale = column(lane_row(jnp.concatenate(lines, axis=0)))
        scale = jnp.concatenate([scale] * (512 // LANES), axis=1)
        for c in range(0, model_dim, 512):
            o = _dot(hidden, wout[:, c:c + 512])
            p = jnp.where(scale > 0.0, scale * o, 0.0).astype(jnp.bfloat16)
            rows_in[first, :, c:c + 512] = p.reshape(PEERS, pair_cap, 512)
        for i in range(PEERS):
            send(rows_in, back_in, relay_b, j, i, -1, back_send, back_recv, relay_b_recv)

    @pl.loop(0, groups)
    def _(j):
        for i in range(PEERS):
            forward(relay_b, back_in, j, i, -1, pass_send, back_recv, relay_b_recv)

    token_ids = lax.broadcasted_iota(jnp.int32, (tok_count, LANES), 0).astype(jnp.float32) + 1.0

    for c in range(0, model_dim, 512):
        acc[:, c:c + 512] = tok[:, c:c + 512].astype(jnp.float32)

    @pl.loop(0, groups)
    def _(j):
        put = (token_ids == asked(j)).astype(jnp.bfloat16)
        arrived(back_in, j, back_recv)
        for c in range(0, model_dim, 512):
            p = back_in[pl.ds(j * PEERS, PEERS), :, c:c + 512].reshape(LANES, 512)
            acc[:, c:c + 512] += _dot(put, p)

    for c in range(0, model_dim, 512):
        out_ref[:, c:c + 512] = acc[:, c:c + 512].astype(out_ref.dtype)

    for src, send_sem in ((ask_out, ask_send), (rows_out, rows_send), (rows_in, back_send)):
        sent = src.at[pl.ds(0, n - 1)]
        pltpu.make_async_copy(sent, sent, send_sem).wait()
    straight = (4 - 1) * (ys - ys // 4) * (zs - zs // 4) * 2
    for relay in (relay_a, relay_b):
        sent = relay.at[pl.ds(0, n - straight)]
        pltpu.make_async_copy(sent, sent, pass_send).wait()


def solution(mesh):
    n = mesh.shape["ep"]
    row_spec = P(("dp", "ep"), None)
    expert_spec = P("ep", None, None)

    def local_layer(tok_loc, sel_loc, gate_loc, win_loc, wout_loc):
        tok_count, model_dim = tok_loc.shape
        ff_dim = win_loc.shape[2]
        pair_cap = LANES // PEERS
        blocks = pltpu.VMEM((n, pair_cap, model_dim), jnp.bfloat16)
        vmem = pl.BlockSpec(memory_space=pltpu.VMEM)
        hbm = pl.BlockSpec(memory_space=pl.ANY)
        return pl.pallas_call(
            functools.partial(moe_kernel, n),
            out_shape=jax.ShapeDtypeStruct((tok_count, model_dim), tok_loc.dtype),
            in_specs=[vmem, vmem, hbm, hbm, hbm],
            out_specs=vmem,
            scratch_shapes=[
                pltpu.VMEM((tok_count, model_dim), jnp.bfloat16),
                pltpu.VMEM((model_dim, ff_dim), jnp.bfloat16),
                pltpu.VMEM((ff_dim, model_dim), jnp.bfloat16),
                pltpu.VMEM((n, 1, LANES), jnp.float32),
                pltpu.VMEM((n, 1, LANES), jnp.float32),
                pltpu.VMEM((n, 1, LANES), jnp.float32),
                blocks, blocks, blocks, blocks, blocks,
                pltpu.VMEM((tok_count, model_dim), jnp.float32),
                pltpu.SemaphoreType.DMA((3,)),
                pltpu.SemaphoreType.DMA,
                pltpu.SemaphoreType.DMA,
                pltpu.SemaphoreType.DMA,
                pltpu.SemaphoreType.DMA((n // PEERS,)),
                pltpu.SemaphoreType.DMA,
                pltpu.SemaphoreType.DMA((n // PEERS,)),
                pltpu.SemaphoreType.DMA((n,)),
                pltpu.SemaphoreType.DMA((n,)),
                pltpu.SemaphoreType.DMA,
            ],
            compiler_params=pltpu.CompilerParams(
                collective_id=0, has_side_effects=True, vmem_limit_bytes=63 * 1024 * 1024),
        )(sel_loc, gate_loc, tok_loc, win_loc[0], wout_loc[0])

    return jax.shard_map(local_layer, mesh=mesh, in_specs=(row_spec, row_spec, row_spec, expert_spec, expert_spec), out_specs=row_spec, check_vma=False)
```

```python
import functools

import jax
import jax.numpy as jnp
from jax import lax
from jax.experimental import pallas as pl
from jax.experimental.pallas import tpu as pltpu
from jax.sharding import PartitionSpec as P

MESH = pl.DeviceIdType.MESH
HIGHEST = lax.Precision.HIGHEST
PEERS = 8
LANES = 128


def _dot(a, b, dims=((1,), (0,)), precision=None):
    return lax.dot_general(a, b, (dims, ((), ())), precision=precision, preferred_element_type=jnp.float32)


def moe_kernel(n, sel_ref, gate_ref, tok_hbm, win_hbm, wout_hbm, out_ref,
               tok, win, wout, ask_out, ask_in, gates, rows_out, rows_in, back_in, relay_a, relay_b, acc,
               load_sem, ask_send, ask_recv, rows_send, rows_recv, back_send, back_recv,
               relay_a_recv, relay_b_recv, pass_send):
    me = lax.axis_index("ep")
    groups = n // PEERS
    pair_cap = LANES // PEERS
    tok_count, model_dim = tok.shape
    slots = sel_ref.shape[1]

    loads = [
        pltpu.make_async_copy(src, dst, load_sem.at[i])
        for i, (src, dst) in enumerate(((tok_hbm, tok), (win_hbm, win), (wout_hbm, wout)))
    ]
    for load in loads:
        load.start()

    ys = min(4, n // 8)
    zs = n // (8 * ys)

    def device(offset, sign):
        dx, dy, dz, core = offset
        x = (me // 2 + 16 + sign * dx) % 4
        y = (me // 8 + 16 + sign * dy) % ys
        z = (me // (8 * ys) + 16 + sign * dz) % zs
        return ((z * ys + y) * 4 + x) * 2 + (me + core) % 2

    def offset_of(j, i):
        t = i // 2
        return t, (j % ys + t) % ys, (j // ys + 4 - t) % zs, i % 2

    def legs(offset, half):
        dx, dy, dz, core = offset
        pair = (dx, 0, 0, 0), (0, dy, dz, core)
        return pair[::-1] if half else pair

    def relayed(offset):
        return offset[0] * (offset[1] + offset[2])

    def halves(model_dim):
        return [pl.ds(h * (model_dim // 2), model_dim // 2) for h in range(2)]

    def send(src, dst, relay, j, i, sign, send_sem, recv_sem, relay_recv):
        slot = j * PEERS + i
        offset = offset_of(j, i)

        @pl.when((relayed(offset) == 0) & (slot > 0))
        def _():
            pltpu.make_async_remote_copy(
                src_ref=src.at[slot], dst_ref=dst.at[slot], send_sem=send_sem, recv_sem=recv_sem.at[j],
                device_id={"ep": device(offset, sign)}, device_id_type=MESH).start()

        @pl.when(relayed(offset) > 0)
        def _():
            for half, columns in enumerate(halves(model_dim)):
                pltpu.make_async_remote_copy(
                    src_ref=src.at[slot, :, columns], dst_ref=relay.at[slot, :, columns],
                    send_sem=send_sem, recv_sem=relay_recv.at[slot],
                    device_id={"ep": device(legs(offset, half)[0], sign)}, device_id_type=MESH).start()

        if i == 0:
            @pl.when(slot == 0)
            def _():
                pltpu.make_async_copy(src.at[slot], dst.at[slot], recv_sem.at[j]).start()

    def forward(relay, dst, j, i, sign, pass_send, recv_sem, relay_recv):
        slot = j * PEERS + i
        offset = offset_of(j, i)

        @pl.when(relayed(offset) > 0)
        def _():
            pltpu.make_async_copy(relay.at[slot], relay.at[slot], relay_recv.at[slot]).wait()
            for half, columns in enumerate(halves(model_dim)):
                pltpu.make_async_remote_copy(
                    src_ref=relay.at[slot, :, columns], dst_ref=dst.at[slot, :, columns],
                    send_sem=pass_send, recv_sem=recv_sem.at[j],
                    device_id={"ep": device(legs(offset, half)[1], sign)}, device_id_type=MESH).start()

    barrier = pltpu.get_barrier_semaphore()

    @pl.loop(1, n)
    def _(k):
        pl.semaphore_signal(barrier, inc=1, device_id={"ep": (me + k) % n}, device_id_type=MESH)

    shift = tok_count.bit_length() - 1
    upper = (lax.broadcasted_iota(jnp.int32, (LANES, LANES), 0)
             < lax.broadcasted_iota(jnp.int32, (LANES, LANES), 1)).astype(jnp.bfloat16)
    lane_of = lax.broadcasted_iota(jnp.int32, (LANES, LANES), 0) % pair_cap
    before = jnp.zeros((n, 1), jnp.float32)
    asks = jnp.zeros((n, LANES), jnp.float32)
    weights = jnp.zeros((n, LANES), jnp.float32)
    for b in range(slots // LANES):
        part = slice(b * LANES, (b + 1) * LANES)
        sel = sel_ref[:, part]
        dev = lax.shift_right_logical(sel, shift)
        row = (sel & (tok_count - 1)).astype(jnp.float32) + 1.0
        hot = lax.broadcasted_iota(jnp.int32, (n, LANES), 0) == dev
        hot_f = hot.astype(jnp.float32)
        count = _dot(hot_f.astype(jnp.bfloat16), upper) + before
        before = before + jnp.sum(hot_f, axis=1, keepdims=True)
        rank = jnp.sum(hot_f * count, axis=0, keepdims=True).astype(jnp.int32)
        mine = lane_of == rank
        asks = asks + _dot(hot_f, jnp.where(mine, row, 0.0), ((1,), (1,)), HIGHEST)
        weights = weights + _dot(hot_f, jnp.where(mine, gate_ref[:, part], 0.0), ((1,), (1,)), HIGHEST)
    gates[...] = weights.reshape(n, 1, LANES)
    ask_out[...] = asks.reshape(n, 1, LANES)

    pl.semaphore_wait(barrier, n - 1)

    @pl.loop(0, groups)
    def _(j):
        for i in range(PEERS):
            slot = j * PEERS + i
            peer = device(offset_of(j, i), -1)

            @pl.when(slot > 0)
            def _():
                pltpu.make_async_remote_copy(
                    src_ref=ask_out.at[peer], dst_ref=ask_in.at[slot], send_sem=ask_send, recv_sem=ask_recv,
                    device_id={"ep": peer}, device_id_type=MESH).start()

    pltpu.make_async_copy(ask_out.at[me], ask_in.at[0], ask_recv).start()
    pltpu.make_async_copy(ask_in, ask_in, ask_recv).wait()
    for load in loads:
        load.wait()

    own_lanes = (lax.broadcasted_iota(jnp.int32, (PEERS, LANES), 1) // pair_cap
                 == lax.broadcasted_iota(jnp.int32, (PEERS, LANES), 0))

    def lane_row(block):
        return jnp.sum(jnp.where(own_lanes, block, 0.0), axis=0, keepdims=True)

    def column(line):
        return jnp.transpose(jnp.broadcast_to(line, (LANES, LANES)))

    def asked(j):
        return lane_row(ask_in[pl.ds(j * PEERS, PEERS)].reshape(PEERS, LANES))

    def arrived(dst, group, recv_sem):
        blocks = dst.at[pl.ds(group * PEERS, PEERS)]
        pltpu.make_async_copy(blocks, blocks, recv_sem.at[group]).wait()

    row_ids = lax.broadcasted_iota(jnp.int32, (LANES, tok_count), 1).astype(jnp.float32) + 1.0

    @pl.loop(0, groups)
    def _(j):
        want = column(asked(j))
        pick = (jnp.concatenate([want] * (tok_count // LANES), axis=1) == row_ids).astype(jnp.bfloat16)
        for c in range(0, model_dim, 512):
            got = _dot(pick, tok[:, c:c + 512]).astype(jnp.bfloat16)
            rows_out[pl.ds(j * PEERS, PEERS), :, c:c + 512] = got.reshape(PEERS, pair_cap, 512)
        for i in range(PEERS):
            send(rows_out, rows_in, relay_a, j, i, 1, rows_send, rows_recv, relay_a_recv)

    @pl.loop(0, groups)
    def _(j):
        for i in range(PEERS):
            forward(relay_a, rows_in, j, i, 1, pass_send, rows_recv, relay_a_recv)

    @pl.loop(0, groups)
    def _(j):
        arrived(rows_in, j, rows_recv)
        first = pl.ds(j * PEERS, PEERS)
        x = rows_in[first].reshape(LANES, model_dim)
        hidden = jax.nn.gelu(_dot(x, win[...]), approximate=True).astype(jnp.bfloat16)
        lines = [gates[device(offset_of(j, i), -1)] for i in range(PEERS)]
        scale = column(lane_row(jnp.concatenate(lines, axis=0)))
        scale = jnp.concatenate([scale] * (512 // LANES), axis=1)
        for c in range(0, model_dim, 512):
            o = _dot(hidden, wout[:, c:c + 512])
            p = jnp.where(scale > 0.0, scale * o, 0.0).astype(jnp.bfloat16)
            rows_in[first, :, c:c + 512] = p.reshape(PEERS, pair_cap, 512)
        for i in range(PEERS):
            send(rows_in, back_in, relay_b, j, i, -1, back_send, back_recv, relay_b_recv)

    @pl.loop(0, groups)
    def _(j):
        for i in range(PEERS):
            forward(relay_b, back_in, j, i, -1, pass_send, back_recv, relay_b_recv)

    token_ids = lax.broadcasted_iota(jnp.int32, (tok_count, LANES), 0).astype(jnp.float32) + 1.0

    for c in range(0, model_dim, 512):
        acc[:, c:c + 512] = tok[:, c:c + 512].astype(jnp.float32)

    @pl.loop(0, groups // 2)
    def _(pair):
        put = []
        for j in (2 * pair, 2 * pair + 1):
            put.append((token_ids == asked(j)).astype(jnp.bfloat16))
            arrived(back_in, j, back_recv)
        put = jnp.concatenate(put, axis=1)
        for c in range(0, model_dim, 512):
            p = back_in[pl.ds(pair * 2 * PEERS, 2 * PEERS), :, c:c + 512].reshape(2 * LANES, 512)
            acc[:, c:c + 512] += _dot(put, p)

    for c in range(0, model_dim, 512):
        out_ref[:, c:c + 512] = acc[:, c:c + 512].astype(out_ref.dtype)

    for src, send_sem in ((ask_out, ask_send), (rows_out, rows_send), (rows_in, back_send)):
        sent = src.at[pl.ds(0, n - 1)]
        pltpu.make_async_copy(sent, sent, send_sem).wait()
    turns = (4 - 1) * (ys * zs - 1) * 2
    for relay in (relay_a, relay_b):
        sent = relay.at[pl.ds(0, turns)]
        pltpu.make_async_copy(sent, sent, pass_send).wait()


def solution(mesh):
    n = mesh.shape["ep"]
    row_spec = P(("dp", "ep"), None)
    expert_spec = P("ep", None, None)

    def local_layer(tok_loc, sel_loc, gate_loc, win_loc, wout_loc):
        tok_count, model_dim = tok_loc.shape
        ff_dim = win_loc.shape[2]
        pair_cap = LANES // PEERS
        blocks = pltpu.VMEM((n, pair_cap, model_dim), jnp.bfloat16)
        vmem = pl.BlockSpec(memory_space=pltpu.VMEM)
        hbm = pl.BlockSpec(memory_space=pl.ANY)
        return pl.pallas_call(
            functools.partial(moe_kernel, n),
            out_shape=jax.ShapeDtypeStruct((tok_count, model_dim), tok_loc.dtype),
            in_specs=[vmem, vmem, hbm, hbm, hbm],
            out_specs=vmem,
            scratch_shapes=[
                pltpu.VMEM((tok_count, model_dim), jnp.bfloat16),
                pltpu.VMEM((model_dim, ff_dim), jnp.bfloat16),
                pltpu.VMEM((ff_dim, model_dim), jnp.bfloat16),
                pltpu.VMEM((n, 1, LANES), jnp.float32),
                pltpu.VMEM((n, 1, LANES), jnp.float32),
                pltpu.VMEM((n, 1, LANES), jnp.float32),
                blocks, blocks, blocks, blocks, blocks,
                pltpu.VMEM((tok_count, model_dim), jnp.float32),
                pltpu.SemaphoreType.DMA((3,)),
                pltpu.SemaphoreType.DMA,
                pltpu.SemaphoreType.DMA,
                pltpu.SemaphoreType.DMA,
                pltpu.SemaphoreType.DMA((n // PEERS,)),
                pltpu.SemaphoreType.DMA,
                pltpu.SemaphoreType.DMA((n // PEERS,)),
                pltpu.SemaphoreType.DMA((n,)),
                pltpu.SemaphoreType.DMA((n,)),
                pltpu.SemaphoreType.DMA,
            ],
            compiler_params=pltpu.CompilerParams(
                collective_id=0, has_side_effects=True, vmem_limit_bytes=63 * 1024 * 1024),
        )(sel_loc, gate_loc, tok_loc, win_loc[0], wout_loc[0])

    return jax.shard_map(local_layer, mesh=mesh, in_specs=(row_spec, row_spec, row_spec, expert_spec, expert_spec), out_specs=row_spec, check_vma=False)
```

```python
import functools

import jax
import jax.numpy as jnp
from jax import lax
from jax.experimental import pallas as pl
from jax.experimental.pallas import tpu as pltpu
from jax.sharding import PartitionSpec as P

MESH = pl.DeviceIdType.MESH
HIGHEST = lax.Precision.HIGHEST
PEERS = 8
LANES = 128


def _dot(a, b, dims=((1,), (0,)), precision=None):
    return lax.dot_general(a, b, (dims, ((), ())), precision=precision, preferred_element_type=jnp.float32)


def moe_kernel(n, sel_ref, gate_ref, tok_hbm, win_hbm, wout_hbm, out_ref,
               tok, win, wout, ask_out, ask_in, gates, rows_out, rows_in, relay_a, relay_b, acc,
               load_sem, ask_send, ask_recv, rows_send, rows_recv, back_send, back_recv,
               relay_a_recv, relay_b_recv, pass_send, ready):
    me = lax.axis_index("ep")
    groups = n // PEERS
    pair_cap = LANES // PEERS
    tok_count, model_dim = tok.shape
    slots = sel_ref.shape[1]

    back_in = rows_out

    loads = [
        pltpu.make_async_copy(src, dst, load_sem.at[i])
        for i, (src, dst) in enumerate(((tok_hbm, tok), (win_hbm, win), (wout_hbm, wout)))
    ]
    for load in loads:
        load.start()

    ys = 4 if n >= 128 else 2
    zs = n // (8 * ys)

    def device(offset, sign):
        dx, dy, dz, core = offset
        x = (me // 2 + 16 + sign * dx) % 4
        y = (me // 8 + 16 + sign * dy) % ys
        z = (me // (8 * ys) + 16 + sign * dz) % zs
        return ((z * ys + y) * 4 + x) * 2 + (me + core) % 2

    def offset_of(j, i):
        t = i // 2
        return t, (j % ys + t) % ys, (j // ys + 4 - t) % zs, i % 2

    def nonzero(d):
        return (d + 3) // 4

    def axes(offset):
        return sum(nonzero(d) for d in offset[:3])

    def way(offset, half):
        order = (2, 1, 0) if half else (0, 1, 2)
        a, b, c = (offset[k] for k in order)
        na, nb, nc = nonzero(a), nonzero(b), nonzero(c)
        first = a, (1 - na) * b, 0
        middle = 0, b, 0
        last = 0, (1 - nc) * b, c

        def placed(leg, core):
            return (*(leg[order.index(k)] for k in range(3)), core)

        return placed(first, 0), placed(middle, 0), placed(last, offset[3])

    halves = [pl.ds(h * (model_dim // 2), model_dim // 2) for h in range(2)]

    def hop(src, dst, slot, half, leg, sign, send_sem, recv_sem):
        pltpu.make_async_remote_copy(
            src_ref=src.at[slot, :, halves[half]], dst_ref=dst.at[slot, :, halves[half]], send_sem=send_sem, recv_sem=recv_sem,
            device_id={"ep": device(leg, sign)}, device_id_type=MESH).start()

    def take(relay, slot, half, recv_sem):
        part = relay.at[slot, :, halves[half]]
        pltpu.make_async_copy(part, part, recv_sem.at[half * n + slot]).wait()

    def straight(src, dst, j, i, sign, send_sem, recv_sem):
        slot = j * PEERS + i
        offset = offset_of(j, i)

        @pl.when((axes(offset) < 2) & (slot > 0))
        def _():
            pltpu.make_async_remote_copy(
                src_ref=src.at[slot], dst_ref=dst.at[slot], send_sem=send_sem, recv_sem=recv_sem.at[j],
                device_id={"ep": device(offset, sign)}, device_id_type=MESH).start()

        if i == 0:
            @pl.when(slot == 0)
            def _():
                pltpu.make_async_copy(src.at[slot], dst.at[slot], recv_sem.at[j]).start()

    def left(src, count, send_sem):
        if count > 0:
            sent = src.at[pl.ds(0, count)]
            pltpu.make_async_copy(sent, sent, send_sem).wait()

    def relays_left():
        left(relay_a, n - 2 * (1 + 3 + ys - 1 + zs - 1), pass_send)
        left(relay_b, 3 * (ys - 1) * (zs - 1) * 2, pass_send)

    def each_half(j, i, bends, body):
        slot = j * PEERS + i
        offset = offset_of(j, i)
        if offset[0] > 0 or bends < 2:
            @pl.when(axes(offset) == bends + 1)
            def _():
                for half in range(2):
                    body(slot, half, way(offset, half))

    barrier = pltpu.get_barrier_semaphore()

    @pl.loop(1, n)
    def _(k):
        pl.semaphore_signal(barrier, inc=1, device_id={"ep": (me + k) % n}, device_id_type=MESH)

    shift = tok_count.bit_length() - 1
    upper = (lax.broadcasted_iota(jnp.int32, (LANES, LANES), 0)
             < lax.broadcasted_iota(jnp.int32, (LANES, LANES), 1)).astype(jnp.bfloat16)
    lane_of = lax.broadcasted_iota(jnp.int32, (LANES, LANES), 0) % pair_cap
    before = jnp.zeros((n, 1), jnp.float32)
    asks = jnp.zeros((n, LANES), jnp.float32)
    weights = jnp.zeros((n, LANES), jnp.float32)
    for b in range(slots // LANES):
        part = slice(b * LANES, (b + 1) * LANES)
        sel = sel_ref[:, part]
        dev = lax.shift_right_logical(sel, shift)
        row = (sel & (tok_count - 1)).astype(jnp.float32) + 1.0
        hot = lax.broadcasted_iota(jnp.int32, (n, LANES), 0) == dev
        hot_f = hot.astype(jnp.float32)
        count = _dot(hot_f.astype(jnp.bfloat16), upper) + before
        before = before + jnp.sum(hot_f, axis=1, keepdims=True)
        rank = jnp.sum(hot_f * count, axis=0, keepdims=True).astype(jnp.int32)
        mine = lane_of == rank
        asks = asks + _dot(hot_f, jnp.where(mine, row, 0.0), ((1,), (1,)), HIGHEST)
        weights = weights + _dot(hot_f, jnp.where(mine, gate_ref[:, part], 0.0), ((1,), (1,)), HIGHEST)
    gates[...] = weights.reshape(n, 1, LANES)
    ask_out[...] = asks.reshape(n, 1, LANES)

    pl.semaphore_wait(barrier, n - 1)

    @pl.loop(0, groups)
    def _(j):
        for i in range(PEERS):
            slot = j * PEERS + i
            peer = device(offset_of(j, i), -1)

            @pl.when(slot > 0)
            def _():
                pltpu.make_async_remote_copy(
                    src_ref=ask_out.at[peer], dst_ref=ask_in.at[slot], send_sem=ask_send, recv_sem=ask_recv,
                    device_id={"ep": peer}, device_id_type=MESH).start()

    pltpu.make_async_copy(ask_out.at[me], ask_in.at[0], ask_recv).start()
    pltpu.make_async_copy(ask_in, ask_in, ask_recv).wait()
    for load in loads:
        load.wait()

    own_lanes = (lax.broadcasted_iota(jnp.int32, (PEERS, LANES), 1) // pair_cap
                 == lax.broadcasted_iota(jnp.int32, (PEERS, LANES), 0))

    def lane_row(block):
        return jnp.sum(jnp.where(own_lanes, block, 0.0), axis=0, keepdims=True)

    def column(line):
        return jnp.transpose(jnp.broadcast_to(line, (LANES, LANES)))

    def asked(j):
        return lane_row(ask_in[pl.ds(j * PEERS, PEERS)].reshape(PEERS, LANES))

    def arrived(dst, group, recv_sem):
        blocks = dst.at[pl.ds(group * PEERS, PEERS)]
        pltpu.make_async_copy(blocks, blocks, recv_sem.at[group]).wait()

    row_ids = lax.broadcasted_iota(jnp.int32, (LANES, tok_count), 1).astype(jnp.float32) + 1.0

    @pl.loop(0, groups)
    def _(j):
        want = column(asked(j))
        pick = (jnp.concatenate([want] * (tok_count // LANES), axis=1) == row_ids).astype(jnp.bfloat16)
        for c in range(0, model_dim, 512):
            got = _dot(pick, tok[:, c:c + 512]).astype(jnp.bfloat16)
            rows_out[pl.ds(j * PEERS, PEERS), :, c:c + 512] = got.reshape(PEERS, pair_cap, 512)
        for i in range(PEERS):
            straight(rows_out, rows_in, j, i, 1, rows_send, rows_recv)

            def start(slot, half, legs):
                hop(rows_out, relay_a, slot, half, legs[0], 1, rows_send, relay_a_recv.at[half * n + slot])

            each_half(j, i, 1, start)
            each_half(j, i, 2, start)

    @pl.loop(0, groups)
    def _(j):
        for i in range(PEERS):
            def finish(slot, half, legs):
                take(relay_a, slot, half, relay_a_recv)
                hop(relay_a, rows_in, slot, half, legs[2], 1, pass_send, rows_recv.at[j])

            def turn(slot, half, legs):
                take(relay_a, slot, half, relay_a_recv)
                hop(relay_a, relay_b, slot, half, legs[1], 1, pass_send, relay_b_recv.at[half * n + slot])

            each_half(j, i, 1, finish)
            each_half(j, i, 2, turn)

    @pl.loop(0, groups)
    def _(j):
        for i in range(PEERS):
            def finish(slot, half, legs):
                take(relay_b, slot, half, relay_b_recv)
                hop(relay_b, rows_in, slot, half, legs[2], 1, pass_send, rows_recv.at[j])

            each_half(j, i, 2, finish)

    left(rows_out, n - 1, rows_send)
    relays_left()
    writers = [(0, 0, 0, 1)]
    for axis, size in enumerate((4, ys, zs)):
        writers += [tuple(d if k == axis else 0 for k in range(3)) + (core,) for d in range(1, size) for core in range(2)]
    for offset in writers:
        pl.semaphore_signal(ready, inc=1, device_id={"ep": device(offset, 1)}, device_id_type=MESH)

    @pl.loop(0, groups)
    def _(j):
        arrived(rows_in, j, rows_recv)
        first = pl.ds(j * PEERS, PEERS)
        x = rows_in[first].reshape(LANES, model_dim)
        hidden = jax.nn.gelu(_dot(x, win[...]), approximate=True).astype(jnp.bfloat16)
        lines = [gates[device(offset_of(j, i), -1)] for i in range(PEERS)]
        scale = column(lane_row(jnp.concatenate(lines, axis=0)))
        scale = jnp.concatenate([scale] * (512 // LANES), axis=1)
        for c in range(0, model_dim, 512):
            o = _dot(hidden, wout[:, c:c + 512])
            p = jnp.where(scale > 0.0, scale * o, 0.0).astype(jnp.bfloat16)
            rows_in[first, :, c:c + 512] = p.reshape(PEERS, pair_cap, 512)

        @pl.when(j == 0)
        def _():
            pl.semaphore_wait(ready, len(writers))

        for i in range(PEERS):
            straight(rows_in, back_in, j, i, -1, back_send, back_recv)

            def start(slot, half, legs):
                hop(rows_in, relay_a, slot, half, legs[2], -1, back_send, relay_a_recv.at[half * n + slot])

            def start_far(slot, half, legs):
                hop(rows_in, relay_b, slot, half, legs[2], -1, back_send, relay_b_recv.at[half * n + slot])

            each_half(j, i, 1, start)
            each_half(j, i, 2, start_far)

    @pl.loop(0, groups)
    def _(j):
        for i in range(PEERS):
            def finish(slot, half, legs):
                take(relay_a, slot, half, relay_a_recv)
                hop(relay_a, back_in, slot, half, legs[0], -1, pass_send, back_recv.at[j])

            def turn(slot, half, legs):
                take(relay_b, slot, half, relay_b_recv)
                hop(relay_b, relay_a, slot, half, legs[1], -1, pass_send, relay_a_recv.at[half * n + slot])

            each_half(j, i, 1, finish)
            each_half(j, i, 2, turn)

    @pl.loop(0, groups)
    def _(j):
        for i in range(PEERS):
            def finish(slot, half, legs):
                take(relay_a, slot, half, relay_a_recv)
                hop(relay_a, back_in, slot, half, legs[0], -1, pass_send, back_recv.at[j])

            each_half(j, i, 2, finish)

    token_ids = lax.broadcasted_iota(jnp.int32, (tok_count, LANES), 0).astype(jnp.float32) + 1.0

    for c in range(0, model_dim, 512):
        acc[:, c:c + 512] = tok[:, c:c + 512].astype(jnp.float32)

    @pl.loop(0, groups // 2)
    def _(pair):
        put = []
        for j in (2 * pair, 2 * pair + 1):
            put.append((token_ids == asked(j)).astype(jnp.bfloat16))
            arrived(back_in, j, back_recv)
        put = jnp.concatenate(put, axis=1)
        for c in range(0, model_dim, 512):
            p = back_in[pl.ds(pair * 2 * PEERS, 2 * PEERS), :, c:c + 512].reshape(2 * LANES, 512)
            acc[:, c:c + 512] += _dot(put, p)

    for c in range(0, model_dim, 512):
        out_ref[:, c:c + 512] = acc[:, c:c + 512].astype(out_ref.dtype)

    left(ask_out, n - 1, ask_send)
    left(rows_in, n - 1, back_send)
    relays_left()


def solution(mesh):
    n = mesh.shape["ep"]
    row_spec = P(("dp", "ep"), None)
    expert_spec = P("ep", None, None)

    def local_layer(tok_loc, sel_loc, gate_loc, win_loc, wout_loc):
        tok_count, model_dim = tok_loc.shape
        ff_dim = win_loc.shape[2]
        pair_cap = LANES // PEERS
        blocks = pltpu.VMEM((n, pair_cap, model_dim), jnp.bfloat16)
        vmem = pl.BlockSpec(memory_space=pltpu.VMEM)
        hbm = pl.BlockSpec(memory_space=pl.ANY)
        return pl.pallas_call(
            functools.partial(moe_kernel, n),
            out_shape=jax.ShapeDtypeStruct((tok_count, model_dim), tok_loc.dtype),
            in_specs=[vmem, vmem, hbm, hbm, hbm],
            out_specs=vmem,
            scratch_shapes=[
                pltpu.VMEM((tok_count, model_dim), jnp.bfloat16),
                pltpu.VMEM((model_dim, ff_dim), jnp.bfloat16),
                pltpu.VMEM((ff_dim, model_dim), jnp.bfloat16),
                pltpu.VMEM((n, 1, LANES), jnp.float32),
                pltpu.VMEM((n, 1, LANES), jnp.float32),
                pltpu.VMEM((n, 1, LANES), jnp.float32),
                blocks, blocks, blocks, blocks,
                pltpu.VMEM((tok_count, model_dim), jnp.float32),
                pltpu.SemaphoreType.DMA((3,)),
                pltpu.SemaphoreType.DMA,
                pltpu.SemaphoreType.DMA,
                pltpu.SemaphoreType.DMA,
                pltpu.SemaphoreType.DMA((n // PEERS,)),
                pltpu.SemaphoreType.DMA,
                pltpu.SemaphoreType.DMA((n // PEERS,)),
                pltpu.SemaphoreType.DMA((2 * n,)),
                pltpu.SemaphoreType.DMA((2 * n,)),
                pltpu.SemaphoreType.DMA,
                pltpu.SemaphoreType.REGULAR,
            ],
            compiler_params=pltpu.CompilerParams(
                collective_id=0, has_side_effects=True, vmem_limit_bytes=63 * 1024 * 1024),
        )(sel_loc, gate_loc, tok_loc, win_loc[0], wout_loc[0])

    return jax.shard_map(local_layer, mesh=mesh, in_specs=(row_spec, row_spec, row_spec, expert_spec, expert_spec), out_specs=row_spec, check_vma=False)
```
